32 devices in a mesh: rep: 8 (over z, x), ep: 4 (over y, core).
Axes of the slice: x: 2, y: 2, z: 4, core: 2. Of those that a mesh axis runs over, the one named last changes fastest.
Arguments:
- tokens: bfloat16 [6144, 2048], P(('rep', 'ep')), may hold values from -6 to 6
- upstream: bfloat16 [6144, 2048], P(('rep', 'ep')), may hold values from -3 to 3
- route_ids: int32 [6144, 2], P(('rep', 'ep')), may hold values from 0 to 3, all different within a row; in each aligned block of 192 rows (0 to 191, 192 to 383, ...) at most 144 rows name the same one
- route_probs: bfloat16 [6144, 2], P(('rep', 'ep')), may hold values from 0.19921875 to 1
- gate_proj: bfloat16 [4, 2048, 768], P('ep'), may hold values from -0.125 to 0.125
- up_proj: bfloat16 [4, 2048, 768], P('ep'), may hold values from -0.125 to 0.125
- down_proj: bfloat16 [4, 768, 2048], P('ep'), may hold values from -0.21875 to 0.21875
Outputs:
- grad_tokens: bfloat16 [6144, 2048], P(('rep', 'ep'))
- grad_probs: bfloat16 [6144, 2], P(('rep', 'ep'))
- grad_gate: float32 [4, 2048, 768], P('ep', 'rep')
- grad_up: float32 [4, 2048, 768], P('ep', 'rep')
- grad_down: float32 [4, 768, 2048], P('ep', None, 'rep')
The draws below stay inside these ranges and needn't reach their ends.
Inputs may be any that keep to these rules, and one draw needn't show every extreme that they name: `route_ids`: each row names 2 different experts. Among the rows of one device no expert is named more than 144 times, and in every draw some expert is named exactly 144 times by the rows of some device.
All inputs are finite; a program needn't handle non-finite values.
Results may differ from the reference program's by a relative error of at most 0.0058.
Values may be sent and summed in bfloat16 or wider, within the bound.
No kernel may reach another device: no remote copies, remote signals or barrier semaphores. Data moves between devices by JAX's collectives and lax.ppermute only.
A program may use at most 128 MiB of HBM per device.

```python
import math
import jax
import jax.numpy as jnp
import numpy as np
from jax import lax

D = 2048
H = 768
TOP = 2
TOK_DEV = 192
EXPERTS = 4
CAP = 144
TOKENS = 6144
N_REP = 8
N_EP = 4


def steps_of(rng, dims, split, low, high):
    level = 1.0
    for position, blocks in split:
        draws = jax.random.uniform(jax.random.fold_in(jax.random.fold_in(rng, 6), position), (blocks,), jnp.float32, low / len(split), high / len(split))
        level = level * jnp.repeat(jnp.exp(draws), dims[position] // blocks).reshape((-1,) + (1,) * (len(dims) - 1 - position))
    return level


def deal_out(stream_key, own, number, rows, number_of, top, most, skew):
    order = jax.random.permutation(stream_key, number_of)
    packed, usual = shares(number_of, rows * top, most, skew, True), shares(number_of, rows * top, most, skew, False)
    places = jnp.arange(number_of)

    def named(sizes, rotation):
        used = int((sizes > 0).sum())
        fixed = max(1, used // 4)
        passed = fixed + (places - fixed + rotation * (used - fixed)) % max(1, number_of - fixed)
        return jnp.zeros((number_of,), jnp.int32).at[order[jnp.where(places < fixed, places, passed)]].set(jnp.asarray(sizes, jnp.int32))

    sizes = jnp.where(number % 4 == 0, named(packed, number // 4), named(usual, number - number // 4 - 1))
    mixed = jax.random.permutation(jax.random.fold_in(own, 3), number_of)
    source_of, sink = mixed[0:number_of // 2 * 2:2], mixed[1:number_of // 2 * 2:2]
    room = jnp.minimum(sizes[source_of] - 1, most - sizes[sink]) // 2
    room = jnp.where((source_of == order[0]) | (sink == order[0]) | (sizes[sink] == 0), 0, jnp.maximum(room, 0))
    passed = jax.random.randint(jax.random.fold_in(own, 4), (number_of // 2,), 0, 1 << 20) % (room + 1)
    sizes = sizes.at[source_of].add(-passed).at[sink].add(passed)
    items = jnp.searchsorted(jnp.cumsum(sizes), jnp.arange(rows * top), side="right").astype(jnp.int32)
    listing = items.reshape(top, rows).T
    listing = listing[jax.random.permutation(jax.random.fold_in(own, 1), rows)]
    rotation = jax.random.randint(jax.random.fold_in(own, 2), (rows, 1), 0, top)
    return jnp.take_along_axis(listing, (jnp.arange(top)[None, :] + rotation) % top, axis=1)


def shares(number_of, total, limit, skew, full):
    loads = [(1 << 20) // math.isqrt(standing ** skew) + 1 for standing in range(1, number_of + 1)]
    largest = limit if full else min(limit, max(-(-total // number_of), total * loads[0] // sum(loads)))
    least = 1 if total - largest >= number_of - 1 else 0
    given, surplus = [largest] + [least] * (number_of - 1), total - largest - least * (number_of - 1)
    while surplus > 0:
        free = [i for i in range(1, number_of) if given[i] < largest] or [i for i in range(1, number_of) if given[i] < limit]
        mass, left = sum([loads[i] for i in free]), surplus
        for i in free:
            addition = min(limit - given[i], max(1, left * loads[i] // mass), surplus)
            given[i] = given[i] + addition
            surplus = surplus - addition
    return np.array(given)


def scatter_about(rng, dims, scale, most, cuts=(), held_as=jnp.bfloat16):
    loudness = steps_of(rng, dims, cuts, -0.22, 0.18) if cuts else 1.0
    entries = jax.random.normal(rng, dims, jnp.float32) * scale * loudness
    return jnp.minimum(jnp.maximum(entries, -most), most).astype(held_as)


def setup_inputs(seed: int = 0) -> dict:
    key_list = jax.random.split(jax.random.key(seed), 8)
    tokens = scatter_about(key_list[0], (TOKENS, D), 1.0, 6.0, ((0, 32),))
    upstream = scatter_about(key_list[1], (TOKENS, D), 0.5, 3.0, ((0, 32),))
    route_ids_keys = jax.random.split(jax.random.fold_in(key_list[2], 1), TOKENS // TOK_DEV)
    route_ids_turns = jax.random.permutation(jax.random.fold_in(key_list[2], 3), TOKENS // TOK_DEV)
    route_ids = jax.vmap(lambda own, number: deal_out(jax.random.fold_in(key_list[2], 2), own, number, TOK_DEV, EXPERTS, TOP, CAP, 1))(route_ids_keys, route_ids_turns).reshape((TOKENS, TOP))
    route_probs = jnp.clip(0.19921875 + 0.80078125 * jax.random.uniform(key_list[3], (TOKENS, TOP), jnp.float32) ** steps_of(key_list[3], (TOKENS, TOP), ((0, 32),), -0.2, 0.2), 0.19921875, 1.0).astype(jnp.bfloat16)
    gate_proj = scatter_about(key_list[4], (EXPERTS, D, H), D ** -0.5, 0.125, ((0, 4),))
    up_proj = scatter_about(key_list[5], (EXPERTS, D, H), D ** -0.5, 0.125, ((0, 4),))
    down_proj = scatter_about(key_list[6], (EXPERTS, H, D), H ** -0.5, 0.21875, ((0, 4),))
    return {"tokens": tokens, "upstream": upstream, "route_ids": route_ids, "route_probs": route_probs, "gate_proj": gate_proj, "up_proj": up_proj, "down_proj": down_proj}


def place_routes(route_block, expert_total, capacity):
    flat_ids = route_block.reshape(-1).astype(jnp.int32)
    onehot = (flat_ids[:, None] == jnp.arange(expert_total, dtype=jnp.int32)[None, :]).astype(jnp.int32)
    before = (jnp.cumsum(onehot, axis=0) - onehot).astype(jnp.int32)
    slot_index = jnp.sum(before * onehot, axis=1).astype(jnp.int32)
    target = (flat_ids * capacity + slot_index).astype(jnp.int32)
    route_total = flat_ids.shape[0]
    source = jnp.zeros((expert_total * capacity,), jnp.int32).at[target].set(jnp.arange(route_total, dtype=jnp.int32))
    filled = jnp.zeros((expert_total * capacity,), jnp.int32).at[target].set(jnp.ones((route_total,), jnp.int32))
    return target, source, filled


def expert_backward(expert_in, expert_up, expert_prob, gate_weight, up_weight, down_weight):
    gate_act = jnp.dot(expert_in, gate_weight, preferred_element_type=jnp.float32)
    up_act = jnp.dot(expert_in, up_weight, preferred_element_type=jnp.float32)
    sigmoid_gate = jax.nn.sigmoid(gate_act)
    silu_gate = gate_act * sigmoid_gate
    activation = silu_gate * up_act
    back_proj = lax.dot_general(expert_up, down_weight, (((1,), (1,)), ((), ())), preferred_element_type=jnp.float32)
    prob_grad = jnp.sum(activation * back_proj, axis=1).astype(jnp.bfloat16)
    prob_col = expert_prob.astype(jnp.float32)[:, None]
    weighted = (prob_col * activation).astype(jnp.bfloat16)
    act_grad = prob_col * back_proj
    gate_grad = (act_grad * up_act * sigmoid_gate * (1.0 + gate_act * (1.0 - sigmoid_gate))).astype(jnp.bfloat16)
    up_grad = (act_grad * silu_gate).astype(jnp.bfloat16)
    routed = lax.dot_general(gate_grad, gate_weight, (((1,), (1,)), ((), ())), preferred_element_type=jnp.float32)
    routed = routed + lax.dot_general(up_grad, up_weight, (((1,), (1,)), ((), ())), preferred_element_type=jnp.float32)
    return gate_grad, up_grad, weighted, routed.astype(jnp.bfloat16), prob_grad


def reference(tokens, upstream, route_ids, route_probs, gate_proj, up_proj, down_proj):
    token_blocks = tokens.reshape(N_REP, N_EP, TOK_DEV, D)
    upstream_blocks = upstream.reshape(N_REP, N_EP, TOK_DEV, D)
    prob_blocks = route_probs.reshape(N_REP, N_EP, TOK_DEV * TOP)
    route_blocks = route_ids.reshape(N_REP, N_EP, TOK_DEV, TOP)

    def placed(route_block):
        return place_routes(route_block, EXPERTS, CAP)

    target, source, filled = jax.vmap(jax.vmap(placed))(route_blocks)
    rep_grid = jnp.broadcast_to(jnp.arange(N_REP, dtype=jnp.int32)[:, None, None], (N_REP, N_EP, CAP))
    ep_grid = jnp.broadcast_to(jnp.arange(N_EP, dtype=jnp.int32)[None, :, None], (N_REP, N_EP, CAP))

    def per_expert(totals, expert):
        token_acc, prob_acc = totals
        slot_source = lax.dynamic_slice_in_dim(source, expert * CAP, CAP, 2)
        live_mask = lax.dynamic_slice_in_dim(filled, expert * CAP, CAP, 2)
        gate_weight = gate_proj[expert]
        up_weight = up_proj[expert]
        down_weight = down_proj[expert]

        def per_replica(sums, replica):
            slot_ids = slot_source[replica]
            keep_mask = live_mask[replica].astype(tokens.dtype)[:, :, None]
            take_rows = jax.vmap(lambda token_block, slot_rows: token_block[slot_rows // TOP])
            expert_in = (take_rows(token_blocks[replica], slot_ids) * keep_mask).reshape(N_EP * CAP, D)
            expert_up = (take_rows(upstream_blocks[replica], slot_ids) * keep_mask).reshape(N_EP * CAP, D)
            take_probs = jax.vmap(lambda prob_block, slot_rows: prob_block[slot_rows])
            expert_prob = (take_probs(prob_blocks[replica], slot_ids) * live_mask[replica].astype(route_probs.dtype)).reshape(-1)
            gate_grad, up_grad, weighted, routed, prob_grad = expert_backward(expert_in, expert_up, expert_prob, gate_weight, up_weight, down_weight)
            contract = (((0,), (0,)), ((), ()))
            gate_total = sums[0] + lax.dot_general(expert_in, gate_grad, contract, preferred_element_type=jnp.float32)
            up_total = sums[1] + lax.dot_general(expert_in, up_grad, contract, preferred_element_type=jnp.float32)
            down_total = sums[2] + lax.dot_general(weighted, expert_up, contract, preferred_element_type=jnp.float32)
            return (gate_total, up_total, down_total), (routed.reshape(N_EP, CAP, D), prob_grad.reshape(N_EP, CAP))

        initial = (jnp.zeros((D, H), jnp.float32), jnp.zeros((D, H), jnp.float32), jnp.zeros((H, D), jnp.float32))
        sums, outputs = lax.scan(per_replica, initial, jnp.arange(N_REP, dtype=jnp.int32))
        routed_all, prob_all = outputs
        mask_float = live_mask.astype(jnp.float32)
        token_acc = token_acc.at[rep_grid, ep_grid, slot_source // TOP].add(routed_all.astype(jnp.float32) * mask_float[:, :, :, None])
        prob_acc = prob_acc.at[rep_grid, ep_grid, slot_source].add(prob_all.astype(jnp.float32) * mask_float)
        rescale = 1.0 / N_REP
        return (token_acc, prob_acc), (sums[0] * rescale, sums[1] * rescale, sums[2] * rescale)

    start = (jnp.zeros((N_REP, N_EP, TOK_DEV, D), jnp.float32), jnp.zeros((N_REP, N_EP, TOK_DEV * TOP), jnp.float32))
    totals, grads = lax.scan(per_expert, start, jnp.arange(EXPERTS, dtype=jnp.int32))
    grad_tokens = totals[0].reshape(TOKENS, D).astype(jnp.bfloat16)
    grad_probs = totals[1].reshape(TOKENS, TOP).astype(jnp.bfloat16)
    return grad_tokens, grad_probs, grads[0], grads[1], grads[2]
```

```python
import jax
import jax.numpy as jnp
from jax import lax
from jax.experimental import pallas as pl
from jax.experimental.pallas import tpu as pltpu
from jax.sharding import PartitionSpec as P


F32 = jnp.float32
BF16 = jnp.bfloat16
ROWS = (((0,), (0,)), ((), ()))
COLS = (((1,), (1,)), ((), ()))


def swap(value, axis, mask):
    count = lax.axis_size(axis)
    return lax.ppermute(value, axis, [(i, i ^ mask) for i in range(count)])


def after(value, *earlier):
    return lax.optimization_barrier((value,) + earlier)[0]


def lane_block(size, most=256):
    return most if size % most == 0 else size


def pick_columns(scalars, offset, count, value, width):
    rows = value.shape[0]

    def kernel(scalar_ref, in_ref, out_ref):
        for k in range(count):
            start = pl.multiple_of(scalar_ref[offset + k] * width, width)
            out_ref[:, k * width : (k + 1) * width] = in_ref[:, pl.ds(start, width)]

    return pl.pallas_call(
        kernel,
        grid_spec=pltpu.PrefetchScalarGridSpec(
            num_scalar_prefetch=1,
            grid=(1,),
            in_specs=[pl.BlockSpec(value.shape, lambda k, t: (0, 0))],
            out_specs=pl.BlockSpec((rows, count * width), lambda k, t: (0, 0)),
        ),
        out_shape=jax.ShapeDtypeStruct((rows, count * width), value.dtype),
    )(scalars, value)


def prob_of(coef_refs, expert):
    parts = []
    for ref in coef_refs:
        lanes = lax.broadcasted_iota(jnp.int32, ref.shape, 1)
        parts.append(jnp.where(lanes == expert, ref[...].astype(F32), 0.0))
    return jnp.sum(jnp.concatenate(parts, axis=0), axis=1, keepdims=True)


def activations(expert, coefs, tokens, gate_w, up_w):
    rows, width = tokens[0].shape
    hidden = gate_w.shape[1]
    total = rows * len(tokens)
    block = lane_block(hidden)
    count = len(tokens)

    def kernel(expert_ref, *refs):
        coef_refs, token_refs = refs[:count], refs[count : 2 * count]
        gate_ref, up_ref, gate_out, up_out, weighted_out, rows_ref = refs[2 * count :]

        @pl.when(pl.program_id(0) == 0)
        def _():
            for j, ref in enumerate(token_refs):
                rows_ref[j * rows : (j + 1) * rows, :] = ref[...]

        x = rows_ref[...]
        gate = jnp.dot(x, gate_ref[...], preferred_element_type=F32)
        up = jnp.dot(x, up_ref[...], preferred_element_type=F32)
        gate_out[...] = gate
        up_out[...] = up
        activation = gate * jax.nn.sigmoid(gate) * up
        weighted_out[...] = (prob_of(coef_refs, expert_ref[0]) * activation).astype(BF16)

    whole = [pl.BlockSpec(c.shape, lambda k, e: (0, 0)) for c in coefs]
    whole += [pl.BlockSpec(t.shape, lambda k, e: (0, 0)) for t in tokens]
    column = pl.BlockSpec((width, block), lambda k, e: (0, k))
    out = pl.BlockSpec((total, block), lambda k, e: (0, k))
    return pl.pallas_call(
        kernel,
        grid_spec=pltpu.PrefetchScalarGridSpec(
            num_scalar_prefetch=1,
            grid=(hidden // block,),
            in_specs=whole + [column, column],
            out_specs=[out, out, out],
            scratch_shapes=[pltpu.VMEM((total, width), BF16)],
        ),
        out_shape=[
            jax.ShapeDtypeStruct((total, hidden), F32),
            jax.ShapeDtypeStruct((total, hidden), F32),
            jax.ShapeDtypeStruct((total, hidden), BF16),
        ],
        cost_estimate=pl.CostEstimate(
            flops=4 * total * width * hidden, bytes_accessed=4 * width * hidden, transcendentals=0
        ),
    )(expert, *coefs, *tokens, gate_w, up_w)


def hidden_grads(scalars, coefs, parts, down_w, gate_act, up_act, own_width):
    rows = parts[0][0].shape[0]
    hidden, width = down_w.shape
    total = rows * len(parts)
    block = lane_block(hidden)
    count = len(parts)
    flat = [part for pair in parts for part in pair]
    per_row = len(parts[0])

    def kernel(scalar_ref, *refs):
        coef_refs, part_refs = refs[:count], refs[count : count + len(flat)]
        down_ref, gate_ref, up_ref, gate_out, up_out, prob_out, rows_ref, sum_ref = refs[count + len(flat) :]
        step = pl.program_id(0)

        @pl.when(step == 0)
        def _():
            for i, ref in enumerate(part_refs):
                j, h = divmod(i, per_row)
                blocks = ref.shape[1] // own_width
                for b in range(blocks):
                    owner = scalar_ref[1 + h * blocks + b]
                    start = pl.multiple_of(owner * own_width, own_width)
                    rows_ref[j * rows : (j + 1) * rows, pl.ds(start, own_width)] = ref[
                        :, b * own_width : (b + 1) * own_width
                    ]
            sum_ref[...] = jnp.zeros_like(sum_ref)

        back = lax.dot_general(rows_ref[...], down_ref[...], COLS, preferred_element_type=F32)
        gate, up = gate_ref[...], up_ref[...]
        s = jax.nn.sigmoid(gate)
        silu = gate * s
        sum_ref[...] += jnp.sum(silu * up * back, axis=1, keepdims=True)
        act_grad = prob_of(coef_refs, scalar_ref[0]) * back
        gate_out[...] = (act_grad * up * s * (1.0 + gate * (1.0 - s))).astype(BF16)
        up_out[...] = (act_grad * silu).astype(BF16)

        @pl.when(step == pl.num_programs(0) - 1)
        def _():
            prob_out[...] = sum_ref[...].astype(BF16)

    whole = [pl.BlockSpec(c.shape, lambda k, e: (0, 0)) for c in coefs]
    whole += [pl.BlockSpec(t.shape, lambda k, e: (0, 0)) for t in flat]
    column = pl.BlockSpec((total, block), lambda k, e: (0, k))
    return pl.pallas_call(
        kernel,
        grid_spec=pltpu.PrefetchScalarGridSpec(
            num_scalar_prefetch=1,
            grid=(hidden // block,),
            in_specs=whole + [pl.BlockSpec((block, width), lambda k, e: (k, 0)), column, column],
            out_specs=[column, column, pl.BlockSpec((total, 1), lambda k, e: (0, 0))],
            scratch_shapes=[pltpu.VMEM((total, width), BF16), pltpu.VMEM((total, 1), F32)],
        ),
        out_shape=[
            jax.ShapeDtypeStruct((total, hidden), BF16),
            jax.ShapeDtypeStruct((total, hidden), BF16),
            jax.ShapeDtypeStruct((total, 1), BF16),
        ],
        cost_estimate=pl.CostEstimate(
            flops=2 * total * width * hidden, bytes_accessed=2 * width * hidden, transcendentals=0
        ),
    )(scalars, *coefs, *flat, down_w, gate_act, up_act)


def weight_blocks(scalars, offset, count, rows, grads, own_width, flip, dtype):
    per_group = len(rows) // len(grads)
    hidden = grads[0].shape[1]
    tok_rows = rows[0].shape[0]
    shape = (hidden, own_width) if flip else (own_width, hidden)

    def kernel(scalar_ref, *refs):
        row_refs, grad_refs, out_ref = refs[: len(rows)], refs[len(rows) : -1], refs[-1]
        where = scalar_ref[offset + pl.program_id(0)] if offset is not None else pl.program_id(0)
        lanes = pl.ds(pl.multiple_of(where * own_width, own_width), own_width)
        acc = None
        for g, grad_ref in enumerate(grad_refs):
            x = jnp.concatenate([r[:, lanes] for r in row_refs[g * per_group : (g + 1) * per_group]], axis=0)
            pair = (grad_ref[...], x) if flip else (x, grad_ref[...])
            term = lax.dot_general(*pair, ROWS, preferred_element_type=F32)
            acc = term if acc is None else acc + term
        out_ref[0] = acc.astype(dtype)

    in_specs = [pl.BlockSpec(x.shape, lambda k, t: (0, 0)) for x in list(rows) + list(grads)]
    return pl.pallas_call(
        kernel,
        grid_spec=pltpu.PrefetchScalarGridSpec(
            num_scalar_prefetch=1,
            grid=(count,),
            in_specs=in_specs,
            out_specs=pl.BlockSpec((1,) + shape, lambda k, t: (k, 0, 0)),
        ),
        out_shape=jax.ShapeDtypeStruct((count,) + shape, dtype),
        cost_estimate=pl.CostEstimate(
            flops=2 * count * own_width * hidden * tok_rows * len(rows),
            bytes_accessed=2 * count * own_width * tok_rows * len(rows),
            transcendentals=0,
        ),
    )(scalars, *rows, *grads)


def masks_of(bits):
    masks = [0]
    for bit in reversed(bits):
        masks = [bit | m for m in masks] + masks
    return masks


def step(tokens, upstream, route_ids, route_probs, gate_proj, up_proj, down_proj):
    ep_count = lax.axis_size("ep")
    rep_count = lax.axis_size("rep")
    ep_index = lax.axis_index("ep")
    rep_index = lax.axis_index("rep")
    tok_rows, model_width = tokens.shape
    own_width = model_width // rep_count
    half = rep_count // 2
    gate_w, up_w, down_w = gate_proj[0], up_proj[0], down_proj[0]
    bits = [1 << i for i in range(rep_count.bit_length() - 1)]
    turned = [bits[1], bits[0]] + bits[2:]
    near_masks, turned_masks = masks_of(bits[1:]), masks_of(turned[1:])
    far_masks, turned_far_masks = [bits[0] | m for m in near_masks], [turned[0] | m for m in turned_masks]
    chip_masks = list(range(0, ep_count, 2))

    lists = far_masks + near_masks + turned_far_masks + turned_masks
    scalars = jnp.concatenate(
        [ep_index.reshape(1).astype(jnp.int32), rep_index ^ jnp.array(lists, jnp.int32)]
    )
    far_at, near_at, turned_far_at, turned_at = (1 + i * half for i in range(4))

    def across(value):
        blocks = {}
        for mask in chip_masks[1:]:
            blocks[mask] = swap(value, "ep", mask)
        blocks[0], blocks[1] = value, swap(value, "ep", 1)
        return blocks

    def forward(blocks, *earlier):
        for mask in chip_masks[1:]:
            blocks[mask] = after(blocks[mask], *earlier)
            blocks[mask | 1] = swap(blocks[mask], "ep", 1)

    token_rows = across(tokens)
    up_far = across(pick_columns(scalars, far_at, half, upstream, own_width))
    up_near = across(pick_columns(scalars, near_at, half, upstream, own_width))
    lanes = jnp.arange(ep_count, dtype=jnp.int32)
    coef = jnp.sum(
        jnp.where(route_ids[:, :, None] == lanes[None, None, :], route_probs[:, :, None].astype(F32), 0.0),
        axis=1,
    ).astype(BF16)
    coefs = {j: swap(coef, "ep", j) if j else coef for j in range(ep_count)}

    acts, grads = {}, {}

    def act(mask, *earlier):
        pair = (mask, mask | 1)
        rows = [token_rows[j] for j in pair]
        rows[0] = after(rows[0], *earlier)
        acts[mask] = activations(scalars, [coefs[j] for j in pair], rows, gate_w, up_w)

    def hidden(mask, *earlier):
        pair = (mask, mask | 1)
        parts = [(up_far[j], up_near[j]) for j in pair]
        grads[mask] = hidden_grads(
            scalars, [coefs[j] for j in pair], parts, down_w, after(acts[mask][0], *earlier), acts[mask][1], own_width
        )

    act(0)
    forward(token_rows, acts[0][0])
    hidden(0)
    forward(up_far, grads[0][0])
    for mask in chip_masks[1:]:
        act(mask, grads[0][0])
    forward(up_near, acts[chip_masks[-1]][0])
    up_far_list = [up_far[j] for j in range(ep_count)]
    token_list = [token_rows[j] for j in range(ep_count)]
    weighted = [acts[mask][2] for mask in chip_masks]

    def outer(offset, rows, grad, flip, dtype):
        return weight_blocks(scalars, offset, half, rows, grad, own_width, flip, dtype)

    down_send = outer(None, up_far_list, weighted, True, BF16)
    down_got = swap(down_send, "rep", bits[0])
    for mask in chip_masks[1:]:
        hidden(mask, down_send)
    up_near_list = [up_near[j] for j in range(ep_count)]
    gate_grads = [grads[mask][0] for mask in chip_masks]
    up_grads = [grads[mask][1] for mask in chip_masks]
    up_send = outer(turned_far_at, token_list, up_grads, False, BF16)
    up_got = swap(up_send, "rep", turned[0])
    gate_grads[0] = after(gate_grads[0], up_send)
    gate_send = outer(far_at, token_list, gate_grads, False, BF16)
    gate_got = swap(gate_send, "rep", bits[0])

    routed = {}
    for mask, gate_grad, up_grad in reversed(list(zip(chip_masks, gate_grads, up_grads))):
        gate_grad = after(gate_grad, gate_send)
        both = lax.dot_general(gate_grad, gate_w, COLS, preferred_element_type=F32)
        both = both + lax.dot_general(up_grad, up_w, COLS, preferred_element_type=F32)
        both = both.astype(BF16)
        routed[mask], routed[mask | 1] = both[:tok_rows], both[tok_rows:]
    back = {mask: swap(routed[mask | 1], "ep", 1) for mask in chip_masks}
    down_keep = outer(None, up_near_list, [after(weighted[0], routed[0])] + weighted[1:], True, F32)
    up_keep = outer(turned_at, token_list, [after(up_grads[0], down_keep)] + up_grads[1:], False, F32)
    sums = {mask: routed[mask].astype(F32) + back[mask].astype(F32) for mask in chip_masks}
    far_sums = [swap(sums[mask].astype(BF16), "ep", mask) for mask in chip_masks[1:]]
    gate_keep = outer(near_at, token_list, [after(gate_grads[0], up_keep)] + gate_grads[1:], False, F32)
    probs_back = []
    for j in range(1, ep_count):
        block = grads[j & ~1][2][(j & 1) * tok_rows : (1 + (j & 1)) * tok_rows]
        probs_back.append(swap(block, "ep", j))

    state = {
        "down": [down_got, down_keep, bits, 0],
        "up": [up_got, up_keep, turned, 0],
        "gate": [gate_got, gate_keep, bits, 0],
    }
    done = [gate_keep]

    def advance(name):
        got, keep, order, at = state[name]
        got = after(got, done[0])
        keep = keep + got.astype(F32)
        if at + 1 == len(order):
            state[name] = keep * (1.0 / rep_count)
            return
        middle = keep.shape[0] // 2
        send = keep[:middle].astype(BF16)
        done[0] = send
        got = swap(send, "rep", order[at + 1])
        state[name] = [got, keep[middle:], order, at + 1]

    advance("down")
    advance("up")
    far_sums = [after(value, done[0]) for value in far_sums]
    token_sum = sums[0]
    for value in far_sums:
        token_sum = token_sum + value.astype(F32)
    grad_tokens = token_sum.astype(BF16)
    own_probs = grads[0][2][:tok_rows]
    grad_probs = 0.0
    for j, block in enumerate([own_probs] + [after(p, done[0]) for p in probs_back]):
        grad_probs = grad_probs + jnp.where(route_ids == ep_index ^ j, block.astype(F32), 0.0)
    levels = range(len(bits))
    events = [(level, 0, "down") for level in levels] + [(level + 1, 2, "gate") for level in levels]
    events += [(level + (level > 0), 1, "up") for level in levels]
    for _, _, name in sorted(events)[2:]:
        advance(name)
    return (grad_tokens, grad_probs.astype(BF16), state["gate"], state["up"], state["down"])


def solution(mesh):
    return jax.shard_map(
        step,
        mesh=mesh,
        in_specs=(
            P(("rep", "ep"), None),
            P(("rep", "ep"), None),
            P(("rep", "ep"), None),
            P(("rep", "ep"), None),
            P("ep", None, None),
            P("ep", None, None),
            P("ep", None, None),
        ),
        out_specs=(
            P(("rep", "ep"), None),
            P(("rep", "ep"), None),
            P("ep", "rep", None),
            P("ep", "rep", None),
            P("ep", None, "rep"),
        ),
        check_vma=False,
    )
```

```python
import jax
import jax.numpy as jnp
from jax import lax
from jax.experimental import pallas as pl
from jax.experimental.pallas import tpu as pltpu
from jax.sharding import PartitionSpec as P


F32 = jnp.float32
BF16 = jnp.bfloat16
ROWS = (((0,), (0,)), ((), ()))
COLS = (((1,), (1,)), ((), ()))


def swap(value, axis, mask):
    count = lax.axis_size(axis)
    return lax.ppermute(value, axis, [(i, i ^ mask) for i in range(count)])


def after(value, *earlier):
    return lax.optimization_barrier((value,) + earlier)[0]


def lane_block(size, most=256):
    return most if size % most == 0 else size


def pick_columns(scalars, masks, value, width):
    rows, count = value.shape[0], len(masks)

    def kernel(scalar_ref, in_ref, out_ref):
        for k, mask in enumerate(masks):
            start = pl.multiple_of((scalar_ref[1] ^ mask) * width, width)
            out_ref[:, k * width : (k + 1) * width] = in_ref[:, pl.ds(start, width)]

    return pl.pallas_call(
        kernel,
        grid_spec=pltpu.PrefetchScalarGridSpec(
            num_scalar_prefetch=1,
            grid=(1,),
            in_specs=[pl.BlockSpec(value.shape, lambda k, t: (0, 0))],
            out_specs=pl.BlockSpec((rows, count * width), lambda k, t: (0, 0)),
        ),
        out_shape=jax.ShapeDtypeStruct((rows, count * width), value.dtype),
    )(scalars, value)


def prob_of(coef_refs, expert):
    parts = []
    for ref in coef_refs:
        lanes = lax.broadcasted_iota(jnp.int32, ref.shape, 1)
        parts.append(jnp.where(lanes == expert, ref[...].astype(F32), 0.0))
    return jnp.sum(jnp.concatenate(parts, axis=0), axis=1, keepdims=True)


def activations(expert, coefs, tokens, gate_w, up_w):
    rows, width = tokens[0].shape
    hidden = gate_w.shape[1]
    total = rows * len(tokens)
    block = lane_block(hidden)
    count = len(tokens)

    def kernel(expert_ref, *refs):
        coef_refs, token_refs = refs[:count], refs[count : 2 * count]
        gate_ref, up_ref, gate_out, up_out, weighted_out, rows_ref = refs[2 * count :]

        @pl.when(pl.program_id(0) == 0)
        def _():
            for j, ref in enumerate(token_refs):
                rows_ref[j * rows : (j + 1) * rows, :] = ref[...]

        x = rows_ref[...]
        gate = jnp.dot(x, gate_ref[...], preferred_element_type=F32)
        up = jnp.dot(x, up_ref[...], preferred_element_type=F32)
        gate_out[...] = gate
        up_out[...] = up
        activation = gate * jax.nn.sigmoid(gate) * up
        weighted_out[...] = (prob_of(coef_refs, expert_ref[0]) * activation).astype(BF16)

    whole = [pl.BlockSpec(c.shape, lambda k, e: (0, 0)) for c in coefs]
    whole += [pl.BlockSpec(t.shape, lambda k, e: (0, 0)) for t in tokens]
    column = pl.BlockSpec((width, block), lambda k, e: (0, k))
    out = pl.BlockSpec((total, block), lambda k, e: (0, k))
    return pl.pallas_call(
        kernel,
        grid_spec=pltpu.PrefetchScalarGridSpec(
            num_scalar_prefetch=1,
            grid=(hidden // block,),
            in_specs=whole + [column, column],
            out_specs=[out, out, out],
            scratch_shapes=[pltpu.VMEM((total, width), BF16)],
        ),
        out_shape=[
            jax.ShapeDtypeStruct((total, hidden), F32),
            jax.ShapeDtypeStruct((total, hidden), F32),
            jax.ShapeDtypeStruct((total, hidden), BF16),
        ],
        cost_estimate=pl.CostEstimate(
            flops=4 * total * width * hidden, bytes_accessed=4 * width * hidden, transcendentals=0
        ),
    )(expert, *coefs, *tokens, gate_w, up_w)


def hidden_grads(scalars, coefs, parts, masks, down_w, gate_act, up_act, own_width):
    rows = parts[0][0].shape[0]
    hidden, width = down_w.shape
    total = rows * len(parts)
    block = lane_block(hidden)
    count = len(parts)
    flat = [part for pair in parts for part in pair]
    groups = len(gate_act)
    per_row = len(parts[0])

    def kernel(scalar_ref, *refs):
        coef_refs, part_refs = refs[:count], refs[count : count + len(flat)]
        rest = refs[count + len(flat) :]
        down_ref, gate_refs, up_refs = rest[0], rest[1 : 1 + groups], rest[1 + groups : 1 + 2 * groups]
        gate_out, up_out, prob_out, rows_ref, sum_ref = rest[1 + 2 * groups :]
        step = pl.program_id(0)

        @pl.when(step == 0)
        def _():
            for i, ref in enumerate(part_refs):
                j, h = divmod(i, per_row)
                blocks = ref.shape[1] // own_width
                for b in range(blocks):
                    owner = scalar_ref[1] ^ masks[h * blocks + b]
                    start = pl.multiple_of(owner * own_width, own_width)
                    rows_ref[j * rows : (j + 1) * rows, pl.ds(start, own_width)] = ref[
                        :, b * own_width : (b + 1) * own_width
                    ]
            sum_ref[...] = jnp.zeros_like(sum_ref)

        back = lax.dot_general(rows_ref[...], down_ref[...], COLS, preferred_element_type=F32)
        gate = jnp.concatenate([r[...] for r in gate_refs], axis=0)
        up = jnp.concatenate([r[...] for r in up_refs], axis=0)
        s = jax.nn.sigmoid(gate)
        silu = gate * s
        sum_ref[...] += jnp.sum(silu * up * back, axis=1, keepdims=True)
        act_grad = prob_of(coef_refs, scalar_ref[0]) * back
        gate_out[...] = (act_grad * up * s * (1.0 + gate * (1.0 - s))).astype(BF16)
        up_out[...] = (act_grad * silu).astype(BF16)

        @pl.when(step == pl.num_programs(0) - 1)
        def _():
            prob_out[...] = sum_ref[...].astype(BF16)

    whole = [pl.BlockSpec(c.shape, lambda k, e: (0, 0)) for c in coefs]
    whole += [pl.BlockSpec(t.shape, lambda k, e: (0, 0)) for t in flat]
    column = pl.BlockSpec((total, block), lambda k, e: (0, k))
    some = [pl.BlockSpec((a.shape[0], block), lambda k, e: (0, k)) for a in gate_act + up_act]
    return pl.pallas_call(
        kernel,
        grid_spec=pltpu.PrefetchScalarGridSpec(
            num_scalar_prefetch=1,
            grid=(hidden // block,),
            in_specs=whole + [pl.BlockSpec((block, width), lambda k, e: (k, 0))] + some,
            out_specs=[column, column, pl.BlockSpec((total, 1), lambda k, e: (0, 0))],
            scratch_shapes=[pltpu.VMEM((total, width), BF16), pltpu.VMEM((total, 1), F32)],
        ),
        out_shape=[
            jax.ShapeDtypeStruct((total, hidden), BF16),
            jax.ShapeDtypeStruct((total, hidden), BF16),
            jax.ShapeDtypeStruct((total, 1), BF16),
        ],
        cost_estimate=pl.CostEstimate(
            flops=2 * total * width * hidden, bytes_accessed=2 * width * hidden, transcendentals=0
        ),
    )(scalars, *coefs, *flat, down_w, *gate_act, *up_act)


def weight_blocks(scalars, masks, rows, grads, own_width, flip, dtype):
    pieces, count = len(masks), len(masks[0])
    hidden = grads[0].shape[1]
    width = hidden // pieces
    piece = (width, own_width) if flip else (own_width, width)
    same = all(m == masks[0] for m in masks)

    def kernel(scalar_ref, *refs):
        row_refs, grad_refs = refs[: len(rows)], refs[len(rows) : len(rows) + len(grads)]
        out_refs = refs[len(rows) + len(grads) :]
        grad = jnp.concatenate([g[...] for g in grad_refs], axis=0)

        def block(k, mask, grad):
            start = k * own_width if flip else (scalar_ref[1] ^ mask) * own_width
            lanes = pl.ds(pl.multiple_of(start, own_width), own_width)
            x = jnp.concatenate([r[:, lanes] for r in row_refs], axis=0)
            pair = (grad, x) if flip else (x, grad)
            return lax.dot_general(*pair, ROWS, preferred_element_type=F32).astype(dtype)

        for k in range(count):
            if same:
                acc = block(k, masks[0][k], grad)
            for i, ref in enumerate(out_refs):
                units = slice(i * width, (i + 1) * width)
                if not same:
                    ref[k] = block(k, masks[i][k], grad[:, units])
                else:
                    ref[k] = acc if pieces == 1 else acc[:, units]

    vmem = pl.BlockSpec(memory_space=pltpu.VMEM)
    return pl.pallas_call(
        kernel,
        in_specs=[pl.BlockSpec(memory_space=pltpu.SMEM)] + [vmem] * (len(rows) + len(grads)),
        out_specs=[vmem] * pieces,
        out_shape=[jax.ShapeDtypeStruct((count,) + piece, dtype)] * pieces,
        cost_estimate=pl.CostEstimate(
            flops=2 * count * own_width * hidden * rows[0].shape[0] * len(rows),
            bytes_accessed=2 * count * own_width * rows[0].shape[0] * len(rows),
            transcendentals=0,
        ),
    )(scalars, *rows, *grads)


def masks_of(bits):
    masks = [0]
    for bit in reversed(bits):
        masks = [bit | m for m in masks] + masks
    return masks


def step(tokens, upstream, route_ids, route_probs, gate_proj, up_proj, down_proj):
    ep_count = lax.axis_size("ep")
    rep_count = lax.axis_size("rep")
    ep_index = lax.axis_index("ep")
    rep_index = lax.axis_index("rep")
    tok_rows, model_width = tokens.shape
    own_width = model_width // rep_count
    gate_w, up_w, down_w = gate_proj[0], up_proj[0], down_proj[0]
    bits = [1 << i for i in range(rep_count.bit_length() - 1)]
    turned = [bits[1], bits[0]] + bits[2:]
    near_masks, turned_masks = masks_of(bits[1:]), masks_of(turned[1:])
    far_masks, turned_far_masks = [bits[0] | m for m in near_masks], [turned[0] | m for m in turned_masks]
    chip_masks = list(range(0, ep_count, 2))

    scalars = jnp.stack([ep_index, rep_index]).astype(jnp.int32)

    def across(value):
        blocks = {}
        for mask in chip_masks[1:]:
            blocks[mask] = swap(value, "ep", mask)
        blocks[0], blocks[1] = value, swap(value, "ep", 1)
        return blocks

    def forward(blocks, *earlier):
        for mask in chip_masks[1:]:
            blocks[mask] = after(blocks[mask], *earlier)
            blocks[mask | 1] = swap(blocks[mask], "ep", 1)

    token_rows = across(tokens)
    lanes = jnp.arange(ep_count, dtype=jnp.int32)
    coef = jnp.sum(
        jnp.where(route_ids[:, :, None] == lanes[None, None, :], route_probs[:, :, None].astype(F32), 0.0),
        axis=1,
    ).astype(BF16)
    coefs = {j: swap(coef, "ep", j) if j else coef for j in range(ep_count)}
    up_far = across(pick_columns(scalars, far_masks, upstream, own_width))
    up_near = across(pick_columns(scalars, near_masks, upstream, own_width))
    acts = {}

    def act(mask, *earlier):
        pair = (mask, mask | 1)
        rows = [token_rows[j] for j in pair]
        rows[0] = after(rows[0], *earlier)
        acts[mask] = activations(scalars, [coefs[j] for j in pair], rows, gate_w, up_w)

    act(0)
    forward(token_rows, acts[0][0])
    for mask in chip_masks[1:]:
        act(mask, acts[0][0])
    forward(up_far, acts[chip_masks[-1]][0])
    up_far_list = [up_far[j] for j in range(ep_count)]
    token_list = [token_rows[j] for j in range(ep_count)]
    weighted = [acts[mask][2] for mask in chip_masks]

    def outer(masks, rows, grad, flip, dtype, *earlier):
        grad = [after(grad[0], *earlier)] + grad[1:] if earlier else grad
        return weight_blocks(scalars, masks, rows, grad, own_width, flip, dtype)

    state = {}

    def send_first(name, values, *orders):
        for i, (value, order) in enumerate(zip(values, orders)):
            state[name, i] = [swap(value, "rep", order[0]), None, order, 0]

    down_send = outer([far_masks], up_far_list, weighted, True, BF16)
    send_first("down", down_send, bits)
    forward(up_near, up_far[1])
    up_near_list = [up_near[j] for j in range(ep_count)]
    gate_acts = [acts[mask][0] for mask in chip_masks]
    gate_acts[0] = after(gate_acts[0], down_send[0])
    gate_grad, up_grad, prob_grad = hidden_grads(
        scalars,
        [coefs[j] for j in range(ep_count)],
        list(zip(up_far_list, up_near_list)),
        far_masks + near_masks,
        down_w,
        gate_acts,
        [acts[mask][1] for mask in chip_masks],
        own_width,
    )
    gate_grads, up_grads = [gate_grad], [up_grad]
    up_send = outer([turned_far_masks, far_masks], token_list, up_grads, False, BF16)
    send_first("up", up_send, turned, bits)
    gate_send = outer([far_masks] * 2, token_list, gate_grads, False, BF16, up_send[0])
    send_first("gate", gate_send, bits, bits)
    down_keep = outer([near_masks], up_near_list, weighted, True, F32, gate_send[0])

    done = [down_keep[0]]

    def advance(name, piece):
        got, keep, order, at = state[name, piece]
        got = after(got, done[0])
        if at + 1 == len(order):
            state[name, piece] = (keep + got.astype(F32)) * (1.0 / rep_count)
            return
        middle = keep.shape[0] // 2
        send = (keep[:middle] + got[:middle].astype(F32)).astype(BF16)
        rest = keep[middle:] + got[middle:].astype(F32)
        done[0] = send
        got = swap(send, "rep", order[at + 1])
        state[name, piece] = [got, rest, order, at + 1]

    def set_keep(name, values):
        for i, value in enumerate(values):
            state[name, i][1] = value
        done[0] = values[-1]

    set_keep("down", down_keep)
    advance("down", 0)
    set_keep("up", outer([turned_masks, near_masks], token_list, up_grads, False, F32, done[0]))
    advance("up", 0)
    set_keep("gate", outer([near_masks] * 2, token_list, gate_grads, False, F32, done[0]))
    advance("gate", 0)

    both = lax.dot_general(after(gate_grad, done[0]), gate_w, COLS, preferred_element_type=F32)
    both = both + lax.dot_general(after(up_grad, done[0]), up_w, COLS, preferred_element_type=F32)
    both = both.astype(BF16).reshape(ep_count, tok_rows, model_width)
    done[0] = both
    back = {mask: swap(both[mask | 1], "ep", 1) for mask in chip_masks}
    prob_blocks = after(prob_grad, done[0]).reshape(ep_count, tok_rows, 1)
    probs_back = [swap(prob_blocks[j], "ep", j) for j in range(1, ep_count)]
    advance("down", 0)
    sums = {}
    for mask in reversed(chip_masks):
        sums[mask] = both[mask].astype(F32) + after(back[mask], done[0]).astype(F32)
    far_sums = [swap(sums[mask].astype(BF16), "ep", mask) for mask in chip_masks[1:]]

    advance("gate", 1)
    advance("gate", 0)
    advance("gate", 1)
    advance("up", 1)
    token_sum = sums[0]
    for value in far_sums:
        token_sum = token_sum + after(value, done[0]).astype(F32)
    grad_tokens = token_sum.astype(BF16)
    grad_probs = 0.0
    for j, block in enumerate([prob_blocks[0]] + [after(p, done[0]) for p in probs_back]):
        grad_probs = grad_probs + jnp.where(route_ids == ep_index ^ j, block.astype(F32), 0.0)
    advance("up", 0)
    advance("up", 1)
    for _ in bits[2:]:
        for name, piece in (("down", 0), ("gate", 0), ("gate", 1), ("up", 0), ("up", 1)):
            advance(name, piece)

    def whole(name):
        return jnp.concatenate([value for key, value in state.items() if key[0] == name], axis=2)

    return (grad_tokens, grad_probs.astype(BF16), whole("gate"), whole("up"), whole("down"))


def solution(mesh):
    return jax.shard_map(
        step,
        mesh=mesh,
        in_specs=(
            P(("rep", "ep"), None),
            P(("rep", "ep"), None),
            P(("rep", "ep"), None),
            P(("rep", "ep"), None),
            P("ep", None, None),
            P("ep", None, None),
            P("ep", None, None),
        ),
        out_specs=(
            P(("rep", "ep"), None),
            P(("rep", "ep"), None),
            P("ep", "rep", None),
            P("ep", "rep", None),
            P("ep", None, "rep"),
        ),
        check_vma=False,
    )
```
